512 devices in a mesh: tm: 8 (over x, core), src: 64 (over y, z).
Axes of the slice: x: 4, y: 8, z: 8, core: 2. Of those that a mesh axis runs over, the one named last changes fastest.
Arguments:
- design: float32 [16, 8388608], P(None, ('tm', 'src')), may hold values from -2 to 2
- unit_index: int32 [8388608], P(('tm', 'src')), may hold values from 0 to 4095, as said below
- residual: float32 [8388608], P(('tm', 'src')), may hold values from -6 to 6
- weight: float32 [8388608], P(('tm', 'src')), may hold values from 0.25 to 4
- obs_count: int32 [512], P(('tm', 'src')), may hold values from 1 to 16384, as said below
- damping: float32 [4096], P(('tm', 'src')), may hold values from 1 to 10
Outputs:
- solution: float32 [16, 4096], P(None, ('tm', 'src'))
- misfit: float32 [], replicated
The draws below stay inside these ranges and needn't reach their ends.
Inputs may be any that keep to these rules, and one draw needn't show every extreme that they name: `unit_index`: an observation on a device of tm index g names a unit in [g * 512, (g + 1) * 512). `obs_count`: some device has all 16384 slots live.
All inputs are finite; a program needn't handle non-finite values.
Results may differ from the reference program's by a relative error of at most 0.0003.
Values sent between devices are 32-bit elements; how exact they have to be, the bound alone decides.
A program may use at most 64 MiB of HBM per device.

```python
import math
import jax
import jax.numpy as jnp
from jax import lax

WIDTH = 16
OBS_DEV = 16384
UNITS_GRP = 512
UNITS = 4096
OBS_ALL = 8388608
N_SRC = 64
DEVICES = 512


def draw_unit_index(key, part):
    total = OBS_DEV * DEVICES
    group = jnp.arange(total, dtype=jnp.int32) // (OBS_DEV * N_SRC)
    picks = jax.random.randint(jax.random.fold_in(key, 11), (total,), 0, UNITS_GRP, dtype=jnp.int32)
    return picks + group * UNITS_GRP


def draw_obs_count(key, part):
    counts = jax.random.randint(jax.random.fold_in(key, 23), (DEVICES,), OBS_DEV // 8, OBS_DEV // 2 + 1, dtype=jnp.int32)
    return counts.at[0].set(OBS_DEV)


def block_scale(stream_key, extent, shards, least, top_value):
    def one(axis_at, blocks):
        steps = jax.random.uniform(jax.random.fold_in(jax.random.fold_in(stream_key, 6), axis_at), (blocks,), jnp.float32, least / len(shards), top_value / len(shards))
        return jnp.repeat(jnp.exp(steps), extent[axis_at] // blocks).reshape((-1,) + (1,) * (len(extent) - axis_at - 1))

    factor_of = one(*shards[0])
    for cut in shards[1:]:
        factor_of = factor_of * one(*cut)
    return factor_of


def bell_draw(own_key, dims, spread, bound, pieces=(), held_as=jnp.bfloat16):
    entries = spread * jax.random.normal(own_key, dims, jnp.float32)
    if pieces:
        entries = entries * block_scale(own_key, dims, pieces, -0.22, 0.18)
    return jnp.clip(entries, -bound, bound).astype(held_as)


def setup_inputs(seed: int = 0) -> dict:
    key_of = jax.random.split(jax.random.key(seed), 7)
    design = bell_draw(key_of[0], (WIDTH, OBS_ALL), 0.25, 2.0, ((1, 512),), jnp.float32)
    unit_index = draw_unit_index(jax.random.fold_in(key_of[6], 71), 0)
    residual = bell_draw(key_of[2], (OBS_ALL,), 1.0, 6.0, ((0, 512),), jnp.float32)
    weight = jnp.clip(jnp.exp(math.log(4.0) - 2.7725887 * jax.random.uniform(key_of[3], (OBS_ALL,), jnp.float32) ** block_scale(key_of[3], (OBS_ALL,), ((0, 512),), -0.2, 0.2)), 0.25, 4.0)
    obs_count = draw_obs_count(jax.random.fold_in(key_of[6], 71), 0)
    damping = jnp.clip(jnp.exp(math.log(10.0) - 2.3025851 * jax.random.uniform(key_of[5], (UNITS,), jnp.float32) ** block_scale(key_of[5], (UNITS,), ((0, 512),), -0.2, 0.2)), 1.0, 10.0)
    return dict(design=design, unit_index=unit_index, residual=residual, weight=weight, obs_count=obs_count, damping=damping)


def block_solve(normal, rhs, damping):
    lower = {}
    for j in range(16):
        running = normal[j * 16 + j] + damping
        for k in range(j):
            running = running - lower[j, k] * lower[j, k]
        diag_term = jnp.sqrt(running)
        lower[j, j] = diag_term
        for i in range(j + 1, 16):
            running = normal[i * 16 + j]
            for k in range(j):
                running = running - lower[i, k] * lower[j, k]
            lower[i, j] = running / diag_term
    forward = []
    for i in range(16):
        running = rhs[i]
        for k in range(i):
            running = running - lower[i, k] * forward[k]
        forward.append(running / lower[i, i])
    backward = [None] * 16
    for i in range(15, -1, -1):
        running = forward[i]
        for k in range(i + 1, 16):
            running = running - lower[k, i] * backward[k]
        backward[i] = running / lower[i, i]
    return jnp.stack(backward)

def reference(design, unit_index, residual, weight, obs_count, damping):
    units = damping.shape[0]
    blocks = obs_count.shape[0]
    design_blocks = design.reshape(16, blocks, -1).transpose(1, 0, 2)
    unit_blocks = unit_index.reshape(blocks, -1)
    resid_blocks = residual.reshape(blocks, -1)
    weight_blocks = weight.reshape(blocks, -1)
    slots = design_blocks.shape[2]

    def accumulate(carry, item):
        normal_sum, rhs_sum, weight_sum = carry
        rows, units_of, resid, weights, count = item
        weights_on = jnp.where(jnp.arange(slots, dtype=jnp.int32) < count, weights, jnp.zeros_like(weights))
        outer = (rows[:, None, :] * rows[None, :, :]).reshape(256, slots) * weights_on
        normal_sum = normal_sum.at[:, units_of].add(outer)
        rhs_sum = rhs_sum.at[:, units_of].add(rows * (weights_on * resid))
        return ((normal_sum, rhs_sum, weight_sum + jnp.sum(weights_on)), None)
    start = (jnp.zeros((256, units), jnp.float32), jnp.zeros((16, units), jnp.float32), jnp.zeros((), jnp.float32))
    (normal, rhs, weight_total), _ = lax.scan(accumulate, start, (design_blocks, unit_blocks, resid_blocks, weight_blocks, obs_count))
    solution = block_solve(normal, rhs, damping)

    def squares(carry, item):
        rows, units_of, resid, weights, count = item
        weights_on = jnp.where(jnp.arange(slots, dtype=jnp.int32) < count, weights, jnp.zeros_like(weights))
        fitted = lax.optimization_barrier(jnp.sum(rows * solution[:, units_of], axis=0))
        after = resid - fitted
        return (carry + jnp.sum(weights_on * after * after), None)
    chi_total, _ = lax.scan(squares, jnp.zeros((), jnp.float32), (design_blocks, unit_blocks, resid_blocks, weight_blocks, obs_count))
    return (solution, chi_total / weight_total)
```

```python
import functools

import jax
import jax.numpy as jnp
from jax import lax
from jax.experimental import pallas as pl
from jax.experimental.pallas import tpu as pltpu
from jax.sharding import PartitionSpec as P

TM = "tm"
SRC = "src"
MESH = pl.DeviceIdType.MESH
W = 16
OWN = 8
BF = jnp.bfloat16
F32 = jnp.float32


def dest_of(m, me, ny, nz):
    own = (ny // 2) * nz + nz // 2
    n = ny * nz
    i = m + (m + (n - own)) // n
    dy = (i // nz + ny // 2) % ny
    dz = (i % nz + nz // 2) % nz
    y = (me // nz + dy) % ny
    z = (me % nz + dz) % nz
    return y * nz + z


def pair_row(i, j):
    s = j - i
    if s < 8:
        return False, s * W + i
    if s == 8:
        return True, i
    return False, (W - s) * W + j


def kernel(
    dims,
    design_ref, unit_ref, resid_ref, weight_ref, count_ref, damping_ref,
    sol_ref, misfit_ref,
    feat, main_acc, rest_acc, sums_acc, main_out, rest_out, main_in, rest_in,
    table, plane_msg, plane_in, tm_msg, tm_in,
    main_send, main_recv, rest_send, rest_recv, plane_send, plane_recv, tm_send, tm_recv,
):
    nt, ny, nz, units, slots, chunk = dims
    n = ny * nz
    me_t = lax.axis_index(TM)
    me_s = lax.axis_index(SRC)

    barrier = pltpu.get_barrier_semaphore()

    def greet(m, carry):
        pl.semaphore_signal(
            barrier, inc=1, device_id=(me_t, dest_of(m, me_s, ny, nz)), device_id_type=MESH
        )
        return carry

    lax.fori_loop(0, n - 1, greet, 0)
    for d in range(1, nt):
        pl.semaphore_signal(
            barrier, inc=1, device_id=((me_t + d) % nt, me_s), device_id_type=MESH
        )

    main_acc[...] = jnp.zeros_like(main_acc)
    rest_acc[...] = jnp.zeros_like(rest_acc)
    sums_acc[...] = jnp.zeros_like(sums_acc)
    feat[...] = jnp.zeros_like(feat)
    count = count_ref[...]
    base = me_t * units
    half = min(units, 256)

    def accumulate(c, carry):
        at = pl.ds(pl.multiple_of(c * chunk, chunk), chunk)
        d = design_ref[:, at]
        slot = lax.broadcasted_iota(jnp.int32, (1, chunk), 1) + c * chunk
        w = jnp.where(slot < count, weight_ref[:, at], 0.0)
        r = resid_ref[:, at]
        wr = w * r
        sums_acc[0:1, :] += wr * r
        sums_acc[1:2, :] += w
        u = unit_ref[:, at] - base
        wd = d * w

        def put(value, row):
            hi = value.astype(BF)
            lo = (value - hi.astype(F32)).astype(BF)
            k = value.shape[0]
            feat[row : row + k, :] = hi
            feat[128 + row : 128 + row + k, :] = lo

        for s in range(8):
            turned = d if s == 0 else pltpu.roll(d, W - s, 0)
            put(wd * turned, s * W)
        tail = jnp.concatenate([wd[:8] * d[8:], d * wr], axis=0)
        tail_hi = tail.astype(BF).astype(F32)
        tail_lo = tail - tail_hi
        quarter = (u // 2) % 4
        for q in range(4):
            on = quarter == q
            feat[256 + q * 32 : 256 + q * 32 + 32, :] = jnp.concatenate(
                [jnp.where(on, tail_hi, 0.0), jnp.zeros((8, chunk), F32)], axis=0
            ).astype(BF)
            feat[384 + q * 32 : 384 + q * 32 + 32, :] = jnp.concatenate(
                [jnp.where(on, tail_lo, 0.0), jnp.zeros((8, chunk), F32)], axis=0
            ).astype(BF)

        def one_hot(index, rows):
            lines = lax.broadcasted_iota(jnp.int32, (rows, chunk), 0).astype(F32).astype(BF)
            return jnp.where(lines == index.astype(F32).astype(BF), jnp.ones((), BF), jnp.zeros((), BF))

        dn = (((1,), (1,)), ((), ()))
        for h in range(units // half):
            main_acc[h * half : (h + 1) * half, :] += lax.dot_general(
                one_hot(u - h * half, half), feat[0:256, :], dn, preferred_element_type=F32
            )
        line = (u // 8) * 2 + u % 2
        rest_acc[...] += lax.dot_general(
            one_hot(line, units // 4), feat[256:512, :], dn, preferred_element_type=F32
        )
        return carry

    lax.fori_loop(0, slots // chunk, accumulate, 0)
    main_out[...] = (main_acc[:, 0:128] + main_acc[:, 128:256]).reshape(n, OWN, 128)
    rest_out[...] = (rest_acc[:, 0:128] + rest_acc[:, 128:256]).reshape(n, 2, 128)

    pl.semaphore_wait(barrier, n - 1 + nt - 1)

    def send(m, carry):
        dest = dest_of(m, me_s, ny, nz)
        pltpu.make_async_remote_copy(
            src_ref=main_out.at[dest], dst_ref=main_in.at[m],
            send_sem=main_send, recv_sem=main_recv,
            device_id=(me_t, dest), device_id_type=MESH,
        ).start()
        pltpu.make_async_remote_copy(
            src_ref=rest_out.at[dest], dst_ref=rest_in.at[m],
            send_sem=rest_send, recv_sem=rest_recv,
            device_id=(me_t, dest), device_id_type=MESH,
        ).start()
        return carry

    lax.fori_loop(0, n - 1, send, 0)
    before = jnp.sum(sums_acc[0:1, :], axis=1, keepdims=True)
    weight_sum = jnp.sum(sums_acc[1:2, :], axis=1, keepdims=True)

    pltpu.make_async_copy(rest_in, rest_in, rest_recv).wait()
    pltpu.make_async_copy(main_in, main_in, main_recv).wait()

    main = main_out[me_s] + jnp.sum(main_in[...], axis=0)
    rest = rest_out[me_s] + jnp.sum(rest_in[...], axis=0)
    table[0:128, :] = jnp.concatenate([main, jnp.zeros((120, 128), F32)], axis=0).T
    rest_t = jnp.concatenate([rest, jnp.zeros((126, 128), F32)], axis=0).T
    lane = lax.broadcasted_iota(jnp.int32, (24, 128), 1)
    rest_all = jnp.zeros((24, 128), F32)
    for q in range(4):
        piece = rest_t[q * 32 : q * 32 + 24, :]
        moved = piece if q == 0 else pltpu.roll(piece, 2 * q, 1)
        rest_all = jnp.where(lane // 2 == q, moved, rest_all)
    table[128:152, :] = rest_all

    def entry(i, j):
        is_rest, row = pair_row(i, j)
        row = row + 128 if is_rest else row
        return table[row : row + 1, 0:OWN]

    damping = damping_ref[...]
    a = {}
    for i in range(W):
        for j in range(i, W):
            a[i, j] = entry(i, j)
        a[i, i] = a[i, i] + damping
    b0 = [table[136 + i : 137 + i, 0:OWN] for i in range(W)]
    b = list(b0)
    inv = [None] * W
    for k in range(W):
        inv[k] = 1.0 / a[k, k]
        for j in range(k + 1, W):
            factor = a[k, j] * inv[k]
            for i in range(k + 1, j + 1):
                a[i, j] = a[i, j] - a[k, i] * factor
            b[j] = b[j] - factor * b[k]
    x = [None] * W
    for k in range(W - 1, -1, -1):
        x[k] = b[k] * inv[k]
        for i in range(k):
            b[i] = b[i] - a[i, k] * x[k]
    gain = jnp.zeros((1, OWN), F32)
    square = jnp.zeros((1, OWN), F32)
    for k in range(W):
        sol_ref[k : k + 1, :] = x[k]
        gain = gain + x[k] * b0[k]
        square = square + x[k] * x[k]
    chi = before - jnp.sum(gain + damping * square, axis=1, keepdims=True)

    lane_row = lax.broadcasted_iota(jnp.int32, (1, 128), 1)
    plane_msg[...] = jnp.where(lane_row == 0, chi, jnp.where(lane_row == 1, weight_sum, 0.0))

    def tell(m, carry):
        dest = dest_of(m, me_s, ny, nz)
        pltpu.make_async_remote_copy(
            src_ref=plane_msg, dst_ref=plane_in.at[m],
            send_sem=plane_send, recv_sem=plane_recv,
            device_id=(me_t, dest), device_id_type=MESH,
        ).start()
        return carry

    lax.fori_loop(0, n - 1, tell, 0)
    pltpu.make_async_copy(plane_in, plane_in, plane_recv).wait()
    tm_msg[...] = plane_msg[...] + jnp.sum(plane_in[...], axis=0)
    for d in range(1, nt):
        pltpu.make_async_remote_copy(
            src_ref=tm_msg, dst_ref=tm_in.at[d - 1],
            send_sem=tm_send, recv_sem=tm_recv,
            device_id=((me_t + d) % nt, me_s), device_id_type=MESH,
        ).start()
    pltpu.make_async_copy(tm_in, tm_in, tm_recv).wait()
    total = tm_msg[...] + jnp.sum(tm_in[...], axis=0)
    misfit_ref[...] = total[:, 0:1] / total[:, 1:2]

    pltpu.make_async_copy(main_in, main_in, main_send).wait()
    pltpu.make_async_copy(rest_in, rest_in, rest_send).wait()
    pltpu.make_async_copy(plane_in, plane_in, plane_send).wait()
    pltpu.make_async_copy(tm_in, tm_in, tm_send).wait()


def solution(mesh):
    nt = mesh.shape[TM]
    n = mesh.shape[SRC]
    nz = 8 if n == 64 else 2
    ny = n // nz
    units = n * OWN

    def on_device(design, unit_index, residual, weight, obs_count, damping):
        slots = design.shape[1]
        chunk = min(2048, slots // 2)
        dims = (nt, ny, nz, units, slots, chunk)
        vmem = pl.BlockSpec(memory_space=pltpu.VMEM)
        dma = pltpu.SemaphoreType.DMA
        sol, misfit = pl.pallas_call(
            functools.partial(kernel, dims),
            out_shape=(
                jax.ShapeDtypeStruct((W, OWN), F32),
                jax.ShapeDtypeStruct((1, 1), F32),
            ),
            in_specs=[vmem] * 6,
            out_specs=(vmem, vmem),
            scratch_shapes=[
                pltpu.VMEM((512, chunk), BF),
                pltpu.VMEM((units, 256), F32),
                pltpu.VMEM((units // 4, 256), F32),
                pltpu.VMEM((2, chunk), F32),
                pltpu.VMEM((n, OWN, 128), F32),
                pltpu.VMEM((n, 2, 128), F32),
                pltpu.VMEM((n - 1, OWN, 128), F32),
                pltpu.VMEM((n - 1, 2, 128), F32),
                pltpu.VMEM((152, 128), F32),
                pltpu.VMEM((1, 128), F32),
                pltpu.VMEM((n - 1, 1, 128), F32),
                pltpu.VMEM((1, 128), F32),
                pltpu.VMEM((nt - 1, 1, 128), F32),
            ] + [dma] * 8,
            compiler_params=pltpu.CompilerParams(collective_id=0, has_side_effects=True),
            name="calibrate",
        )(
            design,
            unit_index.reshape(1, slots),
            residual.reshape(1, slots),
            weight.reshape(1, slots),
            obs_count.reshape(1, 1),
            damping.reshape(1, OWN),
        )
        return sol, misfit.reshape(())

    both = P((TM, SRC))
    return jax.shard_map(
        on_device,
        mesh=mesh,
        in_specs=(P(None, (TM, SRC)), both, both, both, both, both),
        out_specs=(P(None, (TM, SRC)), P()),
        check_vma=False,
    )
```

```python
import functools

import jax
import jax.numpy as jnp
from jax import lax
from jax.experimental import pallas as pl
from jax.experimental.pallas import tpu as pltpu
from jax.sharding import PartitionSpec as P

TM = "tm"
SRC = "src"
MESH = pl.DeviceIdType.MESH
W = 16
OWN = 8
BF = jnp.bfloat16
F32 = jnp.float32


def ring_hops(d, size):
    return min(d, size - d)


def far_first(ny, nz):
    every = [(dy, dz) for dy in range(ny) for dz in range(nz)]
    return sorted(every, key=lambda o: -(ring_hops(o[0], ny) + ring_hops(o[1], nz)))


def pair_row(i, j):
    s = j - i
    if s < 8:
        return False, s * W + i
    if s == 8:
        return True, W + i
    return False, (W - s) * W + j


def kernel(
    dims,
    design_hbm, unit_hbm, resid_hbm, weight_hbm, count_hbm, damping_hbm,
    sol_ref, misfit_ref,
    design_ref, unit_ref, resid_ref, weight_ref, count_ref, damping_ref,
    line_wide, lines, rest_lines,
    feat, rest_feat, main_acc, rest_acc, sums_acc, out_box, in_box,
    table, plane_msg, plane_in, tm_msg, tm_in,
    design_sem, row_sem, box_send, box_recv, plane_send, plane_recv, tm_send, tm_recv,
):
    nt, ny, nz, units, slots, chunk = dims
    n = ny * nz
    turns = slots // chunk
    half_units = units // 2
    half_boxes = n // 2
    me_t = lax.axis_index(TM)
    me_s = lax.axis_index(SRC)
    me_y = me_s // nz
    me_z = me_s % nz

    def piece(c):
        at = pl.ds(pl.multiple_of(c * chunk, chunk), chunk)
        return pltpu.make_async_copy(design_hbm.at[:, at], design_ref.at[:, at], design_sem.at[c])

    rows = [
        pltpu.make_async_copy(a, b, row_sem.at[i])
        for i, (a, b) in enumerate(
            [
                (count_hbm, count_ref), (weight_hbm, weight_ref), (resid_hbm, resid_ref),
                (unit_hbm, unit_ref), (damping_hbm, damping_ref),
            ]
        )
    ]
    for row in rows:
        row.start()
    for c in range(turns):
        piece(c).start()

    ys = [(me_y + d) % ny for d in range(ny)]
    zs = [(me_z + d) % nz for d in range(nz)]
    ts = [(me_t + d) % nt for d in range(nt)]
    order = far_first(ny, nz)

    def owner(o):
        return ys[o[0]] * nz + zs[o[1]]

    def peer(o):
        return (me_t, owner(o))

    barrier = pltpu.get_barrier_semaphore()
    for o in order[:-1]:
        pl.semaphore_signal(barrier, inc=1, device_id=peer(o), device_id_type=MESH)
    for d in range(1, nt):
        pl.semaphore_signal(barrier, inc=1, device_id=(ts[d], me_s), device_id_type=MESH)

    eight = lax.broadcasted_iota(jnp.int32, (OWN, 128), 0)
    for k, o in enumerate(order):
        line_wide[k * OWN : (k + 1) * OWN, :] = (eight + (owner(o) * OWN - 256)).astype(F32)
    lines[...] = line_wide[...].astype(BF)
    for k in range(0, n, 4):
        four = owner(order[k])
        for i in range(1, 4):
            four = jnp.where(eight // 2 == i, owner(order[k + i]), four)
        line_wide[2 * k : 2 * k + OWN, :] = (four * 2 + eight % 2).astype(F32)
    rest_lines[...] = line_wide[0 : 2 * n, :].astype(BF)

    main_acc[...] = jnp.zeros_like(main_acc)
    rest_acc[...] = jnp.zeros_like(rest_acc)
    sums_acc[...] = jnp.zeros_like(sums_acc)
    for row in rows:
        row.wait()
    count = count_ref[0]
    base = me_t * units

    dn = (((1,), (1,)), ((), ()))
    one, zero = jnp.ones((), BF), jnp.zeros((), BF)

    def hits(which, code):
        return jnp.where(
            jnp.concatenate([which] * (chunk // 128), axis=1) == code.astype(F32).astype(BF), one, zero
        )

    def split(value):
        hi = value.astype(BF)
        return hi, (value - hi.astype(F32)).astype(BF)

    def first_half(c, carry):
        at = pl.ds(pl.multiple_of(c * chunk, chunk), chunk)
        piece(c).wait()
        d = design_ref[:, at]
        slot = lax.broadcasted_iota(jnp.int32, (1, chunk), 1) + c * chunk
        w = jnp.where(slot < count, weight_ref[:, at], 0.0)
        r = resid_ref[:, at]
        wr = w * r
        sums_acc[0:1, :] += wr * r
        sums_acc[1:2, :] += w
        u = unit_ref[:, at] - base
        wd = d * w

        for s in range(8):
            turned = d if s == 0 else pltpu.roll(d, W - s, 0)
            hi, lo = split(wd * turned)
            feat[s * W : (s + 1) * W, at] = hi
            feat[128 + s * W : 128 + (s + 1) * W, at] = lo
        tail = jnp.concatenate([d * wr, wd[:8] * d[8:], jnp.zeros((8, chunk), F32)], axis=0)
        tail_hi, tail_lo = split(tail)
        quarter = (lax.shift_right_logical(u, 1) & 3).astype(F32).astype(BF)
        for q in range(4):
            on = quarter == jnp.asarray(q, BF)
            rest_feat[q * 32 : q * 32 + 32, :] = jnp.where(on, tail_hi, zero)
            rest_feat[128 + q * 32 : 160 + q * 32, :] = jnp.where(on, tail_lo, zero)

        code = u - 256
        unit_ref[:, at] = code
        main_acc[0:half_units, :] += lax.dot_general(
            hits(lines[0:half_units, :], code), feat[:, at], dn, preferred_element_type=F32
        )
        rest_code = (lax.shift_right_logical(u, 3) * 2) | (u & 1)
        rest_acc[...] += lax.dot_general(
            hits(rest_lines[...], rest_code), rest_feat[...], dn, preferred_element_type=F32
        )
        return carry

    def second_half(c, carry):
        at = pl.ds(pl.multiple_of(c * chunk, chunk), chunk)
        main_acc[half_units:units, :] += lax.dot_general(
            hits(lines[half_units:units, :], unit_ref[:, at]), feat[:, at], dn, preferred_element_type=F32
        )
        return carry

    def fill(h):
        got = main_acc[h * half_units : (h + 1) * half_units, :]
        out_box[h * half_boxes : (h + 1) * half_boxes, 0:4] = (
            got[:, 0:128] + got[:, 128:256]
        ).reshape(half_boxes, 4, 2, 128)

    def send(h):
        for k in range(h * half_boxes, min((h + 1) * half_boxes, n - 1)):
            pltpu.make_async_remote_copy(
                src_ref=out_box.at[k], dst_ref=in_box.at[k],
                send_sem=box_send.at[h], recv_sem=box_recv.at[h],
                device_id=peer(order[k]), device_id_type=MESH,
            ).start()

    halves = (in_box.at[0:half_boxes], in_box.at[half_boxes : n - 1])

    lax.fori_loop(0, turns, first_half, 0)
    out_box[:, 4:5] = (rest_acc[:, 0:128] + rest_acc[:, 128:256]).reshape(n, 1, 2, 128)
    fill(0)
    pl.semaphore_wait(barrier, n - 1 + nt - 1)
    send(0)
    lax.fori_loop(0, turns, second_half, 0)
    fill(1)
    send(1)

    before = jnp.sum(sums_acc[0:1, :], axis=1, keepdims=True)
    weight_sum = jnp.sum(sums_acc[1:2, :], axis=1, keepdims=True)
    damping = damping_ref[...]
    own = out_box[n - 1]
    pltpu.make_async_copy(halves[0], halves[0], box_recv.at[0]).wait()
    own = own + jnp.sum(in_box[0:half_boxes], axis=0)
    pltpu.make_async_copy(halves[1], halves[1], box_recv.at[1]).wait()
    own = own + jnp.sum(in_box[half_boxes : n - 1], axis=0)
    main = own[0:4].reshape(OWN, 128)
    rest = own[4]
    table[0:128, :] = jnp.concatenate([main, jnp.zeros((120, 128), F32)], axis=0).T
    rest_t = jnp.concatenate([rest, jnp.zeros((126, 128), F32)], axis=0).T
    lane = lax.broadcasted_iota(jnp.int32, (24, 128), 1)
    rest_all = jnp.zeros((24, 128), F32)
    for q in range(4):
        part = rest_t[q * 32 : q * 32 + 24, :]
        moved = part if q == 0 else pltpu.roll(part, 2 * q, 1)
        rest_all = jnp.where(lane // 2 == q, moved, rest_all)
    table[128:152, :] = rest_all

    def entry(i, j):
        is_rest, row = pair_row(i, j)
        row = row + 128 if is_rest else row
        return table[row : row + 1, 0:OWN]

    a = {}
    for i in range(W):
        for j in range(i, W):
            a[i, j] = entry(i, j)
        a[i, i] = a[i, i] + damping
    b0 = [table[128 + i : 129 + i, 0:OWN] for i in range(W)]
    b = list(b0)
    inv = [None] * W
    for k in range(W):
        inv[k] = 1.0 / a[k, k]
        for j in range(k + 1, W):
            factor = a[k, j] * inv[k]
            for i in range(k + 1, j + 1):
                a[i, j] = a[i, j] - a[k, i] * factor
            b[j] = b[j] - factor * b[k]
    x = [None] * W
    for k in range(W - 1, -1, -1):
        x[k] = b[k] * inv[k]
        for i in range(k):
            b[i] = b[i] - a[i, k] * x[k]
    gain = jnp.zeros((1, OWN), F32)
    square = jnp.zeros((1, OWN), F32)
    for k in range(W):
        gain = gain + x[k] * b0[k]
        square = square + x[k] * x[k]
    chi = before - jnp.sum(gain + damping * square, axis=1, keepdims=True)

    lane_row = lax.broadcasted_iota(jnp.int32, (1, 128), 1)
    plane_msg[...] = jnp.where(lane_row == 0, chi, jnp.where(lane_row == 1, weight_sum, 0.0))

    for m, o in enumerate(order[:-1]):
        pltpu.make_async_remote_copy(
            src_ref=plane_msg, dst_ref=plane_in.at[m],
            send_sem=plane_send, recv_sem=plane_recv,
            device_id=peer(o), device_id_type=MESH,
        ).start()
    for k in range(W):
        table[k : k + 1, 0:OWN] = x[k]
    sol_ref[...] = table[...].T[0:OWN, 0:W]
    pltpu.make_async_copy(plane_in, plane_in, plane_recv).wait()
    tm_msg[...] = plane_msg[...] + jnp.sum(plane_in[...], axis=0)
    for d in range(1, nt):
        pltpu.make_async_remote_copy(
            src_ref=tm_msg, dst_ref=tm_in.at[d - 1],
            send_sem=tm_send, recv_sem=tm_recv,
            device_id=(ts[d], me_s), device_id_type=MESH,
        ).start()
    for h in range(2):
        pltpu.make_async_copy(halves[h], halves[h], box_send.at[h]).wait()
    pltpu.make_async_copy(plane_in, plane_in, plane_send).wait()
    pltpu.make_async_copy(tm_in, tm_in, tm_recv).wait()
    total = tm_msg[...] + jnp.sum(tm_in[...], axis=0)
    misfit_ref[...] = total[:, 0:1] / total[:, 1:2]
    pltpu.make_async_copy(tm_in, tm_in, tm_send).wait()


def solution(mesh):
    nt = mesh.shape[TM]
    n = mesh.shape[SRC]
    nz = 8 if n == 64 else 2
    ny = n // nz
    units = n * OWN

    def on_device(design, unit_index, residual, weight, obs_count, damping):
        slots = design.shape[1]
        chunk = min(2048, slots // 2)
        dims = (nt, ny, nz, units, slots, chunk)
        vmem = pl.BlockSpec(memory_space=pltpu.VMEM)
        hbm = pl.BlockSpec(memory_space=pl.ANY)
        dma = pltpu.SemaphoreType.DMA
        sol, misfit = pl.pallas_call(
            functools.partial(kernel, dims),
            out_shape=(
                pltpu.VMEM((OWN, W), F32),
                pltpu.VMEM((1, 1), F32),
            ),
            in_specs=[hbm] * 6,
            out_specs=(vmem, vmem),
            scratch_shapes=[
                pltpu.VMEM((W, slots), F32),
                pltpu.VMEM((1, slots), jnp.int32),
                pltpu.VMEM((1, slots), F32),
                pltpu.VMEM((1, slots), F32),
                pltpu.SMEM((1,), jnp.int32),
                pltpu.VMEM((1, OWN), F32),
                pltpu.VMEM((units, 128), F32),
                pltpu.VMEM((units, 128), BF),
                pltpu.VMEM((units // 4, 128), BF),
                pltpu.VMEM((256, slots), BF),
                pltpu.VMEM((256, chunk), BF),
                pltpu.VMEM((units, 256), F32),
                pltpu.VMEM((units // 4, 256), F32),
                pltpu.VMEM((2, chunk), F32),
                pltpu.VMEM((n, 5, 2, 128), F32),
                pltpu.VMEM((n, 5, 2, 128), F32),
                pltpu.VMEM((152, 128), F32),
                pltpu.VMEM((1, 128), F32),
                pltpu.VMEM((n - 1, 1, 128), F32),
                pltpu.VMEM((1, 128), F32),
                pltpu.VMEM((nt - 1, 1, 128), F32),
                dma((slots // chunk,)),
                dma((5,)),
                dma((2,)),
                dma((2,)),
                dma, dma, dma, dma,
            ],
            compiler_params=pltpu.CompilerParams(collective_id=0, has_side_effects=True),
            name="calibrate",
        )(
            design,
            unit_index.reshape(1, slots),
            residual.reshape(1, slots),
            weight.reshape(1, slots),
            obs_count,
            damping.reshape(1, OWN),
        )
        return sol.T, misfit.reshape(())

    both = P((TM, SRC))
    return jax.shard_map(
        on_device,
        mesh=mesh,
        in_specs=(P(None, (TM, SRC)), both, both, both, both, both),
        out_specs=(P(None, (TM, SRC)), P()),
        check_vma=False,
    )
```

```python
import functools

import jax
import jax.numpy as jnp
from jax import lax
from jax.experimental import pallas as pl
from jax.experimental.pallas import tpu as pltpu
from jax.sharding import PartitionSpec as P

TM = "tm"
SRC = "src"
MESH = pl.DeviceIdType.MESH
W = 16
OWN = 8
BF = jnp.bfloat16
F32 = jnp.float32


def ring_hops(d, size):
    return min(d, size - d)


def far_first(ny, nz):
    every = [(dy, dz) for dy in range(ny) for dz in range(nz)]
    return sorted(every, key=lambda o: -(ring_hops(o[0], ny) + ring_hops(o[1], nz)))


def pair_row(i, j):
    s = j - i
    if s < 8:
        return False, s * W + i
    if s == 8:
        return True, W + i
    return False, (W - s) * W + j


def kernel(
    dims,
    design_hbm, unit_hbm, resid_hbm, weight_hbm, count_hbm, damping_hbm,
    sol_ref, misfit_ref,
    design_ref, unit_ref, resid_ref, weight_ref, count_ref, damping_ref,
    line_wide, lines, rest_lines,
    feat, rest_feat, main_acc, rest_acc, sums_acc, out_box, in_box,
    table, plane_msg, plane_in, tm_msg, tm_in,
    design_sem, row_sem, box_send, box_recv, plane_send, plane_recv, tm_send, tm_recv,
):
    nt, ny, nz, units, slots, chunk = dims
    n = ny * nz
    turns = slots // chunk
    half_units = units // 2
    half_boxes = n // 2
    me_t = lax.axis_index(TM)
    me_s = lax.axis_index(SRC)
    me_y = me_s // nz
    me_z = me_s % nz

    def piece(c):
        at = pl.ds(pl.multiple_of(c * chunk, chunk), chunk)
        return pltpu.make_async_copy(design_hbm.at[:, at], design_ref.at[:, at], design_sem.at[c])

    rows = [
        pltpu.make_async_copy(a, b, row_sem.at[i])
        for i, (a, b) in enumerate(
            [
                (count_hbm, count_ref), (weight_hbm, weight_ref), (resid_hbm, resid_ref),
                (unit_hbm, unit_ref), (damping_hbm, damping_ref),
            ]
        )
    ]
    for row in rows:
        row.start()
    for c in range(turns):
        piece(c).start()

    ys = [(me_y + d) % ny for d in range(ny)]
    zs = [(me_z + d) % nz for d in range(nz)]
    ts = [(me_t + d) % nt for d in range(nt)]
    order = far_first(ny, nz)

    def owner(o):
        return ys[o[0]] * nz + zs[o[1]]

    def peer(o):
        return (me_t, owner(o))

    barrier = pltpu.get_barrier_semaphore()
    for o in order[:-1]:
        pl.semaphore_signal(barrier, inc=1, device_id=peer(o), device_id_type=MESH)
    root_z = 1
    served = nz // root_z - 1
    is_root = me_z < root_z

    @pl.when(is_root)
    def _():
        def greet(place, carry):
            for d in range(1, nt):
                pl.semaphore_signal(barrier, inc=1, device_id=(ts[d], place), device_id_type=MESH)
            return carry

        lax.fori_loop(0, n, greet, 0)

    eight = lax.broadcasted_iota(jnp.int32, (OWN, 128), 0)
    for k, o in enumerate(order):
        line_wide[k * OWN : (k + 1) * OWN, :] = (eight + (owner(o) * OWN - 256)).astype(F32)
    lines[...] = line_wide[...].astype(BF)
    for k in range(0, n, 4):
        four = owner(order[k])
        for i in range(1, 4):
            four = jnp.where(eight // 2 == i, owner(order[k + i]), four)
        line_wide[2 * k : 2 * k + OWN, :] = (four * 2 + eight % 2).astype(F32)
    rest_lines[...] = line_wide[0 : 2 * n, :].astype(BF)

    main_acc[...] = jnp.zeros_like(main_acc)
    rest_acc[...] = jnp.zeros_like(rest_acc)
    sums_acc[...] = jnp.zeros_like(sums_acc)
    for row in rows:
        row.wait()
    count = count_ref[0]
    base = me_t * units

    dn = (((1,), (1,)), ((), ()))
    one, zero = jnp.ones((), BF), jnp.zeros((), BF)

    def hits(which, code):
        return jnp.where(
            jnp.concatenate([which] * (chunk // 128), axis=1) == code.astype(F32).astype(BF), one, zero
        )

    def split(value):
        hi = value.astype(BF)
        return hi, (value - hi.astype(F32)).astype(BF)

    def first_half(c, carry):
        at = pl.ds(pl.multiple_of(c * chunk, chunk), chunk)
        piece(c).wait()
        d = design_ref[:, at]
        slot = lax.broadcasted_iota(jnp.int32, (1, chunk), 1) + c * chunk
        w = jnp.where(slot < count, weight_ref[:, at], 0.0)
        r = resid_ref[:, at]
        wr = w * r
        sums_acc[0:1, :] += wr * r
        sums_acc[1:2, :] += w
        u = unit_ref[:, at] - base
        wd = d * w

        for s in range(8):
            turned = d if s == 0 else pltpu.roll(d, W - s, 0)
            hi, lo = split(wd * turned)
            feat[s * W : (s + 1) * W, at] = hi
            feat[128 + s * W : 128 + (s + 1) * W, at] = lo
        tail = jnp.concatenate([d * wr, wd[:8] * d[8:], jnp.zeros((8, chunk), F32)], axis=0)
        tail_hi, tail_lo = split(tail)
        quarter = jnp.broadcast_to(
            (lax.shift_right_logical(u, 1) & 3).astype(F32), (32, chunk)
        ).astype(BF)
        for q in range(4):
            on = quarter == jnp.asarray(q, BF)
            rest_feat[q * 32 : q * 32 + 32, :] = jnp.where(on, tail_hi, zero)
            rest_feat[128 + q * 32 : 160 + q * 32, :] = jnp.where(on, tail_lo, zero)

        code = u - 256
        unit_ref[:, at] = code
        main_acc[0:half_units, :] += lax.dot_general(
            hits(lines[0:half_units, :], code), feat[:, at], dn, preferred_element_type=F32
        )
        rest_code = (lax.shift_right_logical(u, 3) * 2) | (u & 1)
        rest_acc[...] += lax.dot_general(
            hits(rest_lines[...], rest_code), rest_feat[...], dn, preferred_element_type=F32
        )
        return carry

    def second_half(c, carry):
        at = pl.ds(pl.multiple_of(c * chunk, chunk), chunk)
        main_acc[half_units:units, :] += lax.dot_general(
            hits(lines[half_units:units, :], unit_ref[:, at]), feat[:, at], dn, preferred_element_type=F32
        )
        return carry

    def fill(h):
        got = main_acc[h * half_units : (h + 1) * half_units, :]
        out_box[h * half_boxes : (h + 1) * half_boxes, 0:4] = (
            got[:, 0:128] + got[:, 128:256]
        ).reshape(half_boxes, 4, 2, 128)

    def send(h):
        for k in range(h * half_boxes, min((h + 1) * half_boxes, n - 1)):
            pltpu.make_async_remote_copy(
                src_ref=out_box.at[k], dst_ref=in_box.at[k],
                send_sem=box_send.at[h], recv_sem=box_recv.at[h],
                device_id=peer(order[k]), device_id_type=MESH,
            ).start()

    halves = (in_box.at[0:half_boxes], in_box.at[half_boxes : n - 1])

    lax.fori_loop(0, turns, first_half, 0)
    out_box[:, 4:5] = (rest_acc[:, 0:128] + rest_acc[:, 128:256]).reshape(n, 1, 2, 128)
    fill(0)
    pl.semaphore_wait(barrier, n - 1 + root_z * ny * (nt - 1))
    send(0)
    lax.fori_loop(0, turns, second_half, 0)
    fill(1)
    send(1)

    before = jnp.sum(sums_acc[0:1, :], axis=1, keepdims=True)
    weight_sum = jnp.sum(sums_acc[1:2, :], axis=1, keepdims=True)
    damping = damping_ref[...]
    own = out_box[n - 1]
    pltpu.make_async_copy(halves[0], halves[0], box_recv.at[0]).wait()
    own = own + jnp.sum(in_box[0:half_boxes], axis=0)
    pltpu.make_async_copy(halves[1], halves[1], box_recv.at[1]).wait()
    own = own + jnp.sum(in_box[half_boxes : n - 1], axis=0)
    main = own[0:4].reshape(OWN, 128)
    rest = own[4]
    table[0:128, :] = jnp.concatenate([main, jnp.zeros((120, 128), F32)], axis=0).T
    rest_t = jnp.concatenate([rest, jnp.zeros((126, 128), F32)], axis=0).T
    lane = lax.broadcasted_iota(jnp.int32, (24, 128), 1)
    rest_all = jnp.zeros((24, 128), F32)
    for q in range(4):
        part = rest_t[q * 32 : q * 32 + 24, :]
        moved = part if q == 0 else pltpu.roll(part, 2 * q, 1)
        rest_all = jnp.where(lane // 2 == q, moved, rest_all)
    table[128:152, :] = rest_all

    def entry(i, j):
        is_rest, row = pair_row(i, j)
        row = row + 128 if is_rest else row
        return table[row : row + 1, 0:OWN]

    a = {}
    for i in range(W):
        for j in range(i, W):
            a[i, j] = entry(i, j)
        a[i, i] = a[i, i] + damping
    b0 = [table[128 + i : 129 + i, 0:OWN] for i in range(W)]
    b = list(b0)
    inv = [None] * W
    for k in range(W):
        inv[k] = 1.0 / a[k, k]
        for j in range(k + 1, W):
            factor = a[k, j] * inv[k]
            for i in range(k + 1, j + 1):
                a[i, j] = a[i, j] - a[k, i] * factor
            b[j] = b[j] - factor * b[k]
    x = [None] * W
    for k in range(W - 1, -1, -1):
        x[k] = b[k] * inv[k]
        for i in range(k):
            b[i] = b[i] - a[i, k] * x[k]
    gain = jnp.zeros((1, OWN), F32)
    square = jnp.zeros((1, OWN), F32)
    for k in range(W):
        gain = gain + x[k] * b0[k]
        square = square + x[k] * x[k]
    chi = before - jnp.sum(gain + damping * square, axis=1, keepdims=True)

    lane_row = lax.broadcasted_iota(jnp.int32, (1, 128), 1)
    plane_msg[...] = jnp.where(lane_row == 0, chi, jnp.where(lane_row == 1, weight_sum, 0.0))

    def term_copy(d, dy, z):
        slot = (nt - d) % nt * n + (ny - dy) % ny * nz + (me_z - z + nz) % nz
        return pltpu.make_async_remote_copy(
            src_ref=plane_msg, dst_ref=plane_in.at[slot],
            send_sem=plane_send, recv_sem=plane_recv,
            device_id=(ts[d], ys[dy] * nz + z), device_id_type=MESH,
        )

    ways = sorted(
        ((d, dy) for d in range(nt) for dy in range(ny)),
        key=lambda w: -(ring_hops(w[0] // 2, nt // 2) + ring_hops(w[1], ny)),
    )
    for d, dy in ways:
        for z in range(root_z):
            if (d, dy) != (0, 0):
                term_copy(d, dy, z).start()
    for z in range(root_z):

        @pl.when(me_z != z)
        def _():
            term_copy(0, 0, z).start()

    for k in range(W):
        table[k : k + 1, 0:OWN] = x[k]
    sol_ref[...] = table[...].T[0:OWN, 0:W]
    every = n * nt - 1
    to_roots = root_z * ny * nt

    def total_copy(i):
        z = me_z * (root_z + i) + (1 - me_z) * (nz - 1 - i)
        return pltpu.make_async_remote_copy(
            src_ref=tm_msg, dst_ref=tm_in,
            send_sem=tm_send, recv_sem=tm_recv,
            device_id=(me_t, me_y * nz + z), device_id_type=MESH,
        )

    def finish(total):
        misfit_ref[0, 0] = jnp.sum(total[:, 0:1] / total[:, 1:2])

    def drain(count, sem):
        pltpu.make_async_copy(plane_in.at[0:count], plane_in.at[0:count], sem).wait()

    @pl.when(is_root)
    def _():
        drain(every, plane_recv)
        plane_in[0] = plane_msg[...]
        total = jnp.sum(plane_in[...], axis=0)
        tm_msg[...] = total
        for i in range(served):
            total_copy(i).start()
        finish(total)
        drain(to_roots - 1, plane_send)
        drain(served, tm_send)

    @pl.when(jnp.logical_not(is_root))
    def _():
        pltpu.make_async_copy(tm_in, tm_in, tm_recv).wait()
        finish(tm_in[...])
        drain(to_roots, plane_send)

    for h in range(2):
        pltpu.make_async_copy(halves[h], halves[h], box_send.at[h]).wait()


def solution(mesh):
    nt = mesh.shape[TM]
    n = mesh.shape[SRC]
    nz = 8 if n == 64 else 2
    ny = n // nz
    units = n * OWN

    def on_device(design, unit_index, residual, weight, obs_count, damping):
        slots = design.shape[1]
        chunk = min(4096, slots // 2)
        dims = (nt, ny, nz, units, slots, chunk)
        vmem = pl.BlockSpec(memory_space=pltpu.VMEM)
        hbm = pl.BlockSpec(memory_space=pl.ANY)
        dma = pltpu.SemaphoreType.DMA
        sol, misfit = pl.pallas_call(
            functools.partial(kernel, dims),
            out_shape=(
                pltpu.VMEM((OWN, W), F32),
                pltpu.SMEM((1, 1), F32),
            ),
            in_specs=[hbm] * 6,
            out_specs=(vmem, pl.BlockSpec(memory_space=pltpu.SMEM)),
            scratch_shapes=[
                pltpu.VMEM((W, slots), F32),
                pltpu.VMEM((1, slots), jnp.int32),
                pltpu.VMEM((1, slots), F32),
                pltpu.VMEM((1, slots), F32),
                pltpu.SMEM((1,), jnp.int32),
                pltpu.VMEM((1, OWN), F32),
                pltpu.VMEM((units, 128), F32),
                pltpu.VMEM((units, 128), BF),
                pltpu.VMEM((units // 4, 128), BF),
                pltpu.VMEM((256, slots), BF),
                pltpu.VMEM((256, chunk), BF),
                pltpu.VMEM((units, 256), F32),
                pltpu.VMEM((units // 4, 256), F32),
                pltpu.VMEM((2, chunk), F32),
                pltpu.VMEM((n, 5, 2, 128), F32),
                pltpu.VMEM((n, 5, 2, 128), F32),
                pltpu.VMEM((152, 128), F32),
                pltpu.VMEM((1, 128), F32),
                pltpu.VMEM((n * nt, 1, 128), F32),
                pltpu.VMEM((1, 128), F32),
                pltpu.VMEM((1, 128), F32),
                dma((slots // chunk,)),
                dma((5,)),
                dma((2,)),
                dma((2,)),
                dma, dma, dma, dma,
            ],
            compiler_params=pltpu.CompilerParams(collective_id=0, has_side_effects=True),
            name="calibrate",
        )(
            design,
            unit_index.reshape(1, slots),
            residual.reshape(1, slots),
            weight.reshape(1, slots),
            obs_count,
            damping.reshape(1, OWN),
        )
        return sol.T, misfit.reshape(())

    both = P((TM, SRC))
    return jax.shard_map(
        on_device,
        mesh=mesh,
        in_specs=(P(None, (TM, SRC)), both, both, both, both, both),
        out_specs=(P(None, (TM, SRC)), P()),
        check_vma=False,
    )
```

```python
import functools

import jax
import jax.numpy as jnp
from jax import lax
from jax.experimental import pallas as pl
from jax.experimental.pallas import tpu as pltpu
from jax.sharding import PartitionSpec as P

TM = "tm"
SRC = "src"
MESH = pl.DeviceIdType.MESH
W = 16
OWN = 8
BF = jnp.bfloat16
F32 = jnp.float32


def ring_hops(d, size):
    return min(d, size - d)


def far_first(ny, nz):
    every = [(dy, dz) for dy in range(ny) for dz in range(nz)]
    return sorted(every, key=lambda o: -(ring_hops(o[0], ny) + ring_hops(o[1], nz)))


def pair_row(i, j):
    s = j - i
    if s < 8:
        return False, s * W + i
    if s == 8:
        return True, W + i
    return False, (W - s) * W + j


def tree_sum(parts):
    while len(parts) > 1:
        parts = [sum(parts[i : i + 2][1:], parts[i]) for i in range(0, len(parts), 2)]
    return parts[0]


def kernel(
    dims,
    design_hbm, unit_hbm, resid_hbm, weight_hbm, count_hbm, damping_hbm,
    sol_ref, misfit_ref,
    design_ref, unit_ref, resid_ref, weight_ref, count_ref, damping_ref,
    line_wide, lines, rest_lines,
    feat, rest_feat, main_acc, rest_acc, sums_acc, out_box, in_box,
    table, plane_msg, plane_in, tm_msg, tm_in,
    design_sem, row_sem, box_send, box_recv, plane_send, plane_recv, tm_send, tm_recv,
):
    nt, ny, nz, units, slots, chunk = dims
    n = ny * nz
    turns = slots // chunk
    half_units = units // 2
    half_boxes = n // 2
    me_t = lax.axis_index(TM)
    me_s = lax.axis_index(SRC)
    me_y = me_s // nz
    me_z = me_s % nz

    def piece(c):
        at = pl.ds(pl.multiple_of(c * chunk, chunk), chunk)
        return pltpu.make_async_copy(design_hbm.at[:, at], design_ref.at[:, at], design_sem.at[c])

    rows = [
        pltpu.make_async_copy(a, b, row_sem.at[i])
        for i, (a, b) in enumerate(
            [
                (count_hbm, count_ref), (weight_hbm, weight_ref), (resid_hbm, resid_ref),
                (unit_hbm, unit_ref), (damping_hbm, damping_ref),
            ]
        )
    ]
    for row in rows:
        row.start()
    for c in range(turns):
        piece(c).start()

    ys = [(me_y + d) % ny for d in range(ny)]
    zs = [(me_z + d) % nz for d in range(nz)]
    ts = [(me_t + d) % nt for d in range(nt)]
    order = far_first(ny, nz)

    def owner(o):
        return ys[o[0]] * nz + zs[o[1]]

    def peer(o):
        return (me_t, owner(o))

    barrier = pltpu.get_barrier_semaphore()
    for o in order[:-1]:
        pl.semaphore_signal(barrier, inc=1, device_id=peer(o), device_id_type=MESH)
    root_z = 1
    served = nz // root_z - 1
    is_root = me_z < root_z

    @pl.when(is_root)
    def _():
        def greet(place, carry):
            for d in range(1, nt):
                pl.semaphore_signal(barrier, inc=1, device_id=(ts[d], place), device_id_type=MESH)
            return carry

        lax.fori_loop(0, n, greet, 0)

    eight = lax.broadcasted_iota(jnp.int32, (OWN, 128), 0)
    for k, o in enumerate(order):
        line_wide[k * OWN : (k + 1) * OWN, :] = (eight + (owner(o) * OWN - 256)).astype(F32)
    lines[...] = line_wide[...].astype(BF)
    for k in range(0, n, 4):
        four = owner(order[k])
        for i in range(1, 4):
            four = jnp.where(eight // 2 == i, owner(order[k + i]), four)
        line_wide[2 * k : 2 * k + OWN, :] = (four * 2 + eight % 2).astype(F32)
    rest_lines[...] = line_wide[0 : 2 * n, :].astype(BF)

    main_acc[...] = jnp.zeros_like(main_acc)
    rest_acc[...] = jnp.zeros_like(rest_acc)
    sums_acc[...] = jnp.zeros_like(sums_acc)
    for row in rows:
        row.wait()
    count = count_ref[0]
    base = me_t * units

    dn = (((1,), (1,)), ((), ()))
    one, zero = jnp.ones((), BF), jnp.zeros((), BF)

    def hits(which, code):
        return jnp.where(
            jnp.concatenate([which] * (chunk // 128), axis=1) == code.astype(F32).astype(BF), one, zero
        )

    def split(value):
        hi = value.astype(BF)
        return hi, (value - hi.astype(F32)).astype(BF)

    def first_half(c, carry):
        at = pl.ds(pl.multiple_of(c * chunk, chunk), chunk)
        piece(c).wait()
        d = design_ref[:, at]
        slot = lax.broadcasted_iota(jnp.int32, (1, chunk), 1) + c * chunk
        w = jnp.where(slot < count, weight_ref[:, at], 0.0)
        r = resid_ref[:, at]
        wr = w * r
        sums_acc[0:1, :] += wr * r
        sums_acc[1:2, :] += w
        u = unit_ref[:, at] - base
        wd = d * w

        for s in range(8):
            turned = d if s == 0 else pltpu.roll(d, W - s, 0)
            hi, lo = split(wd * turned)
            feat[s * W : (s + 1) * W, at] = hi
            feat[128 + s * W : 128 + (s + 1) * W, at] = lo
        tail = jnp.concatenate([d * wr, wd[:8] * d[8:]], axis=0)
        tail_hi, tail_lo = split(tail)
        quarter = jnp.broadcast_to(
            (lax.shift_right_logical(u, 1) & 3).astype(F32), (24, chunk)
        ).astype(BF)
        for q in range(4):
            on = quarter == jnp.asarray(q, BF)
            rest_feat[q * 24 : q * 24 + 24, :] = jnp.where(on, tail_hi, zero)
            rest_feat[96 + q * 24 : 120 + q * 24, :] = jnp.where(on, tail_lo, zero)

        code = u - 256
        unit_ref[:, at] = code
        main_acc[0:half_units, :] += lax.dot_general(
            hits(lines[0:half_units, :], code), feat[:, at], dn, preferred_element_type=F32
        )
        rest_code = (lax.shift_right_logical(u, 3) * 2) | (u & 1)
        rest_acc[:, 0:192] += lax.dot_general(
            hits(rest_lines[...], rest_code), rest_feat[...], dn, preferred_element_type=F32
        )
        return carry

    def second_half(c, carry):
        at = pl.ds(pl.multiple_of(c * chunk, chunk), chunk)
        main_acc[half_units:units, :] += lax.dot_general(
            hits(lines[half_units:units, :], unit_ref[:, at]), feat[:, at], dn, preferred_element_type=F32
        )
        return carry

    def fill(h):
        got = main_acc[h * half_units : (h + 1) * half_units, :]
        out_box[h * half_boxes : (h + 1) * half_boxes, 0:4] = (
            got[:, 0:128] + got[:, 128:256]
        ).reshape(half_boxes, 4, 2, 128)

    def send(h):
        for k in range(h * half_boxes, min((h + 1) * half_boxes, n - 1)):
            pltpu.make_async_remote_copy(
                src_ref=out_box.at[k], dst_ref=in_box.at[k],
                send_sem=box_send.at[h], recv_sem=box_recv.at[h],
                device_id=peer(order[k]), device_id_type=MESH,
            ).start()

    halves = (in_box.at[0:half_boxes], in_box.at[half_boxes : n - 1])

    lax.fori_loop(0, turns, first_half, 0)
    out_box[:, 4:5] = (
        rest_acc[:, 0:128] + pltpu.roll(rest_acc[...], 160, 1)[:, 0:128]
    ).reshape(n, 1, 2, 128)
    fill(0)
    pl.semaphore_wait(barrier, n - 1 + root_z * ny * (nt - 1))
    send(0)
    lax.fori_loop(0, turns, second_half, 0)
    fill(1)
    send(1)

    before = jnp.sum(sums_acc[0:1, :], axis=1, keepdims=True)
    weight_sum = jnp.sum(sums_acc[1:2, :], axis=1, keepdims=True)
    damping = damping_ref[...]
    own = out_box[n - 1]
    pltpu.make_async_copy(halves[0], halves[0], box_recv.at[0]).wait()
    own = tree_sum([own] + [in_box[k] for k in range(half_boxes)])
    pltpu.make_async_copy(halves[1], halves[1], box_recv.at[1]).wait()
    own = tree_sum([own] + [in_box[k] for k in range(half_boxes, n - 1)])
    main = own[0:4].reshape(OWN, 128)
    rest = own[4]
    table[0:128, :] = jnp.concatenate([main, jnp.zeros((120, 128), F32)], axis=0).T
    rest_t = jnp.concatenate([rest, jnp.zeros((126, 128), F32)], axis=0).T
    lane = lax.broadcasted_iota(jnp.int32, (24, 128), 1)
    rest_all = jnp.zeros((24, 128), F32)
    for q in range(4):
        part = rest_t[q * 24 : q * 24 + 24, :]
        moved = part if q == 0 else pltpu.roll(part, 2 * q, 1)
        rest_all = jnp.where(lane // 2 == q, moved, rest_all)
    table[128:152, :] = rest_all

    def entry(i, j):
        is_rest, row = pair_row(i, j)
        row = row + 128 if is_rest else row
        return table[row : row + 1, 0:OWN]

    a = {}
    for i in range(W):
        for j in range(i, W):
            a[i, j] = entry(i, j)
        a[i, i] = a[i, i] + damping
    b0 = [table[128 + i : 129 + i, 0:OWN] for i in range(W)]
    b = list(b0)
    inv = [None] * W
    for k in range(W):
        inv[k] = 1.0 / a[k, k]
        for j in range(k + 1, W):
            factor = a[k, j] * inv[k]
            for i in range(k + 1, j + 1):
                a[i, j] = a[i, j] - a[k, i] * factor
            b[j] = b[j] - factor * b[k]
    x = [None] * W
    for k in range(W - 1, -1, -1):
        x[k] = b[k] * inv[k]
        for i in range(k):
            b[i] = b[i] - a[i, k] * x[k]
    gain = jnp.zeros((1, OWN), F32)
    square = jnp.zeros((1, OWN), F32)
    for k in range(W):
        gain = gain + x[k] * b0[k]
        square = square + x[k] * x[k]
    chi = before - jnp.sum(gain + damping * square, axis=1, keepdims=True)

    lane_row = lax.broadcasted_iota(jnp.int32, (1, 128), 1)
    plane_msg[...] = jnp.where(lane_row == 0, chi, jnp.where(lane_row == 1, weight_sum, 0.0))

    def term_copy(d, dy, z):
        slot = (nt - d) % nt * n + (ny - dy) % ny * nz + (me_z - z + nz) % nz
        return pltpu.make_async_remote_copy(
            src_ref=plane_msg, dst_ref=plane_in.at[pl.ds(slot, 1)],
            send_sem=plane_send, recv_sem=plane_recv,
            device_id=(ts[d], ys[dy] * nz + z), device_id_type=MESH,
        )

    ways = sorted(
        ((d, dy) for d in range(nt) for dy in range(ny)),
        key=lambda w: -(ring_hops(w[0] // 2, nt // 2) + ring_hops(w[1], ny)),
    )
    for d, dy in ways:
        for z in range(root_z):
            if (d, dy) != (0, 0):
                term_copy(d, dy, z).start()
    for z in range(root_z):

        @pl.when(me_z != z)
        def _():
            term_copy(0, 0, z).start()

    for k in range(W):
        table[k : k + 1, 0:OWN] = x[k]
    sol_ref[...] = table[...].T[0:OWN, 0:W]
    every = n * nt - 1
    to_roots = root_z * ny * nt

    def total_copy(i):
        z = me_z * (root_z + i) + (1 - me_z) * (nz - 1 - i)
        return pltpu.make_async_remote_copy(
            src_ref=tm_msg, dst_ref=tm_in,
            send_sem=tm_send, recv_sem=tm_recv,
            device_id=(me_t, me_y * nz + z), device_id_type=MESH,
        )

    def finish(total):
        misfit_ref[0, 0] = jnp.sum(total[:, 0:1] / total[:, 1:2])

    def drain(count, sem):
        pltpu.make_async_copy(plane_in.at[pl.ds(0, count)], plane_in.at[pl.ds(0, count)], sem).wait()

    @pl.when(is_root)
    def _():
        drain(every, plane_recv)
        plane_in[0:1] = plane_msg[...]
        eights = tree_sum([plane_in[8 * k : 8 * k + 8, :] for k in range(n * nt // 8)])
        total = jnp.sum(eights, axis=0, keepdims=True)
        tm_msg[...] = total
        for i in range(served):
            total_copy(i).start()
        finish(total)
        drain(to_roots - 1, plane_send)
        drain(served, tm_send)

    @pl.when(jnp.logical_not(is_root))
    def _():
        pltpu.make_async_copy(tm_in, tm_in, tm_recv).wait()
        finish(tm_in[...])
        drain(to_roots, plane_send)

    for h in range(2):
        pltpu.make_async_copy(halves[h], halves[h], box_send.at[h]).wait()


def solution(mesh):
    nt = mesh.shape[TM]
    n = mesh.shape[SRC]
    nz = 8 if n == 64 else 2
    ny = n // nz
    units = n * OWN

    def on_device(design, unit_index, residual, weight, obs_count, damping):
        slots = design.shape[1]
        chunk = min(4096, slots // 2)
        dims = (nt, ny, nz, units, slots, chunk)
        vmem = pl.BlockSpec(memory_space=pltpu.VMEM)
        hbm = pl.BlockSpec(memory_space=pl.ANY)
        dma = pltpu.SemaphoreType.DMA
        sol, misfit = pl.pallas_call(
            functools.partial(kernel, dims),
            out_shape=(
                pltpu.VMEM((OWN, W), F32),
                pltpu.SMEM((1, 1), F32),
            ),
            in_specs=[hbm] * 6,
            out_specs=(vmem, pl.BlockSpec(memory_space=pltpu.SMEM)),
            scratch_shapes=[
                pltpu.VMEM((W, slots), F32),
                pltpu.VMEM((1, slots), jnp.int32),
                pltpu.VMEM((1, slots), F32),
                pltpu.VMEM((1, slots), F32),
                pltpu.SMEM((1,), jnp.int32),
                pltpu.VMEM((1, OWN), F32),
                pltpu.VMEM((units, 128), F32),
                pltpu.VMEM((units, 128), BF),
                pltpu.VMEM((units // 4, 128), BF),
                pltpu.VMEM((256, slots), BF),
                pltpu.VMEM((192, chunk), BF),
                pltpu.VMEM((units, 256), F32),
                pltpu.VMEM((units // 4, 256), F32),
                pltpu.VMEM((2, chunk), F32),
                pltpu.VMEM((n, 5, 2, 128), F32),
                pltpu.VMEM((n, 5, 2, 128), F32),
                pltpu.VMEM((152, 128), F32),
                pltpu.VMEM((1, 128), F32),
                pltpu.VMEM((n * nt, 128), F32),
                pltpu.VMEM((1, 128), F32),
                pltpu.VMEM((1, 128), F32),
                dma((slots // chunk,)),
                dma((5,)),
                dma((2,)),
                dma((2,)),
                dma, dma, dma, dma,
            ],
            compiler_params=pltpu.CompilerParams(collective_id=0, has_side_effects=True),
            name="calibrate",
        )(
            design,
            unit_index.reshape(1, slots),
            residual.reshape(1, slots),
            weight.reshape(1, slots),
            obs_count,
            damping.reshape(1, OWN),
        )
        return sol.T, misfit.reshape(())

    both = P((TM, SRC))
    return jax.shard_map(
        on_device,
        mesh=mesh,
        in_specs=(P(None, (TM, SRC)), both, both, both, both, both),
        out_specs=(P(None, (TM, SRC)), P()),
        check_vma=False,
    )
```

```python
import functools

import jax
import jax.numpy as jnp
from jax import lax
from jax.experimental import pallas as pl
from jax.experimental.pallas import tpu as pltpu
from jax.sharding import PartitionSpec as P

TM = "tm"
SRC = "src"
MESH = pl.DeviceIdType.MESH
W = 16
OWN = 8
BF = jnp.bfloat16
F32 = jnp.float32


def ring_hops(d, size):
    return min(d, size - d)


def far_first(ny, nz):
    every = [(dy, dz) for dy in range(ny) for dz in range(nz)]
    return sorted(every, key=lambda o: -(ring_hops(o[0], ny) + ring_hops(o[1], nz)))


def pair_row(i, j):
    s = j - i
    if s < 8:
        return False, s * W + i
    if s == 8:
        return True, W + i
    return False, (W - s) * W + j


def tree_sum(parts):
    while len(parts) > 1:
        parts = [sum(parts[i : i + 2][1:], parts[i]) for i in range(0, len(parts), 2)]
    return parts[0]


def kernel(
    dims,
    design_hbm, unit_hbm, resid_hbm, weight_hbm, count_hbm, damping_hbm,
    sol_ref, misfit_ref,
    design_ref, unit_ref, resid_ref, weight_ref, count_ref, damping_ref,
    line_wide, lines, rest_lines,
    feat, rest_feat, main_acc, rest_acc, sums_acc, out_box, in_box,
    table, plane_msg, plane_in, tm_msg, tm_in,
    design_sem, row_sem, box_send, box_recv, plane_send, plane_recv, tm_send, tm_recv,
):
    nt, ny, nz, units, slots, chunk = dims
    n = ny * nz
    turns = slots // chunk
    half_units = units // 2
    half_boxes = n // 2
    me_t = lax.axis_index(TM)
    me_s = lax.axis_index(SRC)
    me_y = me_s // nz
    me_z = me_s % nz

    def piece(c):
        at = pl.ds(pl.multiple_of(c * chunk, chunk), chunk)
        return pltpu.make_async_copy(design_hbm.at[:, at], design_ref.at[:, at], design_sem.at[c])

    rows = [
        pltpu.make_async_copy(a, b, row_sem.at[i])
        for i, (a, b) in enumerate(
            [
                (count_hbm, count_ref), (weight_hbm, weight_ref), (resid_hbm, resid_ref),
                (unit_hbm, unit_ref), (damping_hbm, damping_ref),
            ]
        )
    ]
    for row in rows:
        row.start()
    for c in range(turns):
        piece(c).start()

    ys = [(me_y + d) % ny for d in range(ny)]
    zs = [(me_z + d) % nz for d in range(nz)]
    ts = [(me_t + d) % nt for d in range(nt)]
    order = far_first(ny, nz)

    def owner(o):
        return ys[o[0]] * nz + zs[o[1]]

    def peer(o):
        return (me_t, owner(o))

    barrier = pltpu.get_barrier_semaphore()
    for o in order[:-1]:
        pl.semaphore_signal(barrier, inc=1, device_id=peer(o), device_id_type=MESH)
    root_z = 1
    served = nz // root_z - 1
    is_root = me_z < root_z

    @pl.when(is_root)
    def _():
        def greet(place, carry):
            for d in range(1, nt):
                pl.semaphore_signal(barrier, inc=1, device_id=(ts[d], place), device_id_type=MESH)
            return carry

        lax.fori_loop(0, n, greet, 0)

    eight = lax.broadcasted_iota(jnp.int32, (OWN, 128), 0)
    for k, o in enumerate(order):
        line_wide[k * OWN : (k + 1) * OWN, :] = (eight + (owner(o) * OWN - 256)).astype(F32)
    lines[...] = line_wide[...].astype(BF)
    for k in range(0, n, 4):
        four = owner(order[k])
        for i in range(1, 4):
            four = jnp.where(eight // 2 == i, owner(order[k + i]), four)
        line_wide[2 * k : 2 * k + OWN, :] = (four * 2 + eight % 2).astype(F32)
    rest_lines[...] = line_wide[0 : 2 * n, :].astype(BF)

    main_acc[...] = jnp.zeros_like(main_acc)
    rest_acc[...] = jnp.zeros_like(rest_acc)
    sums_acc[...] = jnp.zeros_like(sums_acc)
    for row in rows:
        row.wait()
    count = count_ref[0]
    base = me_t * units

    dn = (((1,), (1,)), ((), ()))
    one, zero = jnp.ones((), BF), jnp.zeros((), BF)

    def hits(which, code):
        return jnp.where(
            jnp.concatenate([which] * (chunk // 128), axis=1) == code.astype(F32).astype(BF), one, zero
        )

    def split(value):
        hi = value.astype(BF)
        return hi, (value - hi.astype(F32)).astype(BF)

    def first_half(c, carry):
        at = pl.ds(pl.multiple_of(c * chunk, chunk), chunk)
        piece(c).wait()
        d = design_ref[:, at]
        slot = lax.broadcasted_iota(jnp.int32, (1, chunk), 1) + c * chunk
        w = jnp.where(slot < count, weight_ref[:, at], 0.0)
        r = resid_ref[:, at]
        wr = w * r
        sums_acc[0:1, :] += wr * r
        sums_acc[1:2, :] += w
        u = unit_ref[:, at] - base
        wd = d * w

        for s in range(8):
            turned = d if s == 0 else pltpu.roll(d, W - s, 0)
            hi, lo = split(wd * turned)
            feat[s * W : (s + 1) * W, at] = hi
            feat[128 + s * W : 128 + (s + 1) * W, at] = lo
        tail = jnp.concatenate([d * wr, wd[:8] * d[8:]], axis=0)
        tail_hi, tail_lo = split(tail)
        quarter = jnp.broadcast_to(
            (lax.shift_right_logical(u, 1) & 3).astype(F32), (24, chunk)
        ).astype(BF)
        for q in range(4):
            on = quarter == jnp.asarray(q, BF)
            rest_feat[q * 24 : q * 24 + 24, :] = jnp.where(on, tail_hi, zero)
            rest_feat[96 + q * 24 : 120 + q * 24, :] = jnp.where(on, tail_lo, zero)

        code = u - 256
        unit_ref[:, at] = code
        main_acc[0:half_units, :] += lax.dot_general(
            hits(lines[0:half_units, :], code), feat[:, at], dn, preferred_element_type=F32
        )
        rest_code = (lax.shift_right_logical(u, 3) * 2) | (u & 1)
        rest_acc[:, 0:192] += lax.dot_general(
            hits(rest_lines[...], rest_code), rest_feat[...], dn, preferred_element_type=F32
        )
        return carry

    def second_half(c, carry):
        at = pl.ds(pl.multiple_of(c * chunk, chunk), chunk)
        main_acc[half_units:units, :] += lax.dot_general(
            hits(lines[half_units:units, :], unit_ref[:, at]), feat[:, at], dn, preferred_element_type=F32
        )
        return carry

    def fill(h):
        got = main_acc[h * half_units : (h + 1) * half_units, :]
        out_box[h * half_boxes : (h + 1) * half_boxes, 0:4] = (
            got[:, 0:128] + got[:, 128:256]
        ).reshape(half_boxes, 4, 2, 128)

    def send(h):
        for k in range(h * half_boxes, min((h + 1) * half_boxes, n - 1)):
            pltpu.make_async_remote_copy(
                src_ref=out_box.at[k], dst_ref=in_box.at[k],
                send_sem=box_send.at[h], recv_sem=box_recv.at[h],
                device_id=peer(order[k]), device_id_type=MESH,
            ).start()

    halves = (in_box.at[0:half_boxes], in_box.at[half_boxes : n - 1])

    lax.fori_loop(0, turns, first_half, 0)
    out_box[:, 4:5] = (
        rest_acc[:, 0:128] + pltpu.roll(rest_acc[...], 160, 1)[:, 0:128]
    ).reshape(n, 1, 2, 128)
    fill(0)
    pl.semaphore_wait(barrier, n - 1 + root_z * ny * (nt - 1))
    send(0)
    lax.fori_loop(0, turns, second_half, 0)
    fill(1)
    send(1)

    before = jnp.sum(sums_acc[0:1, :], axis=1, keepdims=True)
    weight_sum = jnp.sum(sums_acc[1:2, :], axis=1, keepdims=True)
    lane_row = lax.broadcasted_iota(jnp.int32, (1, 128), 1)
    plane_msg[...] = jnp.where(
        lane_row == OWN, before, jnp.where(lane_row == OWN + 1, weight_sum, 0.0)
    )
    damping = damping_ref[...]
    own = out_box[n - 1]
    pltpu.make_async_copy(halves[0], halves[0], box_recv.at[0]).wait()
    own = tree_sum([own] + [in_box[k] for k in range(half_boxes)])
    pltpu.make_async_copy(halves[1], halves[1], box_recv.at[1]).wait()
    own = tree_sum([own] + [in_box[k] for k in range(half_boxes, n - 1)])
    main = own[0:4].reshape(OWN, 128)
    rest = own[4]
    table[0:128, :] = jnp.concatenate([main, jnp.zeros((120, 128), F32)], axis=0).T
    rest_t = jnp.concatenate([rest, jnp.zeros((126, 128), F32)], axis=0).T
    lane = lax.broadcasted_iota(jnp.int32, (24, 128), 1)
    rest_all = jnp.zeros((24, 128), F32)
    for q in range(4):
        part = rest_t[q * 24 : q * 24 + 24, :]
        moved = part if q == 0 else pltpu.roll(part, 2 * q, 1)
        rest_all = jnp.where(lane // 2 == q, moved, rest_all)
    table[128:152, :] = rest_all

    def entry(i, j):
        is_rest, row = pair_row(i, j)
        row = row + 128 if is_rest else row
        return table[row : row + 1, 0:OWN]

    a = {}
    for i in range(W):
        for j in range(i, W):
            a[i, j] = entry(i, j)
        a[i, i] = a[i, i] + damping
    b0 = [table[128 + i : 129 + i, 0:OWN] for i in range(W)]
    b = list(b0)
    inv = [None] * W
    for k in range(W):
        inv[k] = 1.0 / a[k, k]
        for j in range(k + 1, W):
            factor = a[k, j] * inv[k]
            for i in range(k + 1, j + 1):
                a[i, j] = a[i, j] - a[k, i] * factor
            b[j] = b[j] - factor * b[k]
    x = [None] * W
    for k in range(W - 1, -1, -1):
        x[k] = b[k] * inv[k]
        for i in range(k):
            b[i] = b[i] - a[i, k] * x[k]
    gain = jnp.zeros((1, OWN), F32)
    square = jnp.zeros((1, OWN), F32)
    for k in range(W):
        gain = gain + x[k] * b0[k]
        square = square + x[k] * x[k]
    plane_msg[:, 0:OWN] = -(gain + damping * square)

    def term_copy(d, dy, z):
        slot = (nt - d) % nt * n + (ny - dy) % ny * nz + (me_z - z + nz) % nz
        return pltpu.make_async_remote_copy(
            src_ref=plane_msg, dst_ref=plane_in.at[pl.ds(slot, 1)],
            send_sem=plane_send, recv_sem=plane_recv,
            device_id=(ts[d], ys[dy] * nz + z), device_id_type=MESH,
        )

    ways = sorted(
        ((d, dy) for d in range(nt) for dy in range(ny)),
        key=lambda w: -(ring_hops(w[0] // 2, nt // 2) + ring_hops(w[1], ny)),
    )
    for d, dy in ways:
        for z in range(root_z):
            if (d, dy) != (0, 0):
                term_copy(d, dy, z).start()
    for z in range(root_z):

        @pl.when(me_z != z)
        def _():
            term_copy(0, 0, z).start()

    for k in range(W):
        table[k : k + 1, 0:OWN] = x[k]
    sol_ref[...] = table[...].T[0:OWN, 0:W]
    every = n * nt - 1
    to_roots = root_z * ny * nt

    def total_copy(i):
        z = me_z * (root_z + i) + (1 - me_z) * (nz - 1 - i)
        return pltpu.make_async_remote_copy(
            src_ref=tm_msg, dst_ref=tm_in,
            send_sem=tm_send, recv_sem=tm_recv,
            device_id=(me_t, me_y * nz + z), device_id_type=MESH,
        )

    def finish(total):
        chi = jnp.sum(jnp.where(lane_row <= OWN, total, 0.0), axis=1, keepdims=True)
        weights = jnp.sum(jnp.where(lane_row == OWN + 1, total, 0.0), axis=1, keepdims=True)
        misfit_ref[0, 0] = jnp.sum(chi / weights)

    def drain(count, sem):
        pltpu.make_async_copy(plane_in.at[pl.ds(0, count)], plane_in.at[pl.ds(0, count)], sem).wait()

    @pl.when(is_root)
    def _():
        drain(every, plane_recv)
        plane_in[0:1] = plane_msg[...]
        eights = tree_sum([plane_in[8 * k : 8 * k + 8, :] for k in range(n * nt // 8)])
        total = jnp.sum(eights, axis=0, keepdims=True)
        tm_msg[...] = total
        for i in range(served):
            total_copy(i).start()
        finish(total)
        drain(to_roots - 1, plane_send)
        drain(served, tm_send)

    @pl.when(jnp.logical_not(is_root))
    def _():
        pltpu.make_async_copy(tm_in, tm_in, tm_recv).wait()
        finish(tm_in[...])
        drain(to_roots, plane_send)

    for h in range(2):
        pltpu.make_async_copy(halves[h], halves[h], box_send.at[h]).wait()


def solution(mesh):
    nt = mesh.shape[TM]
    n = mesh.shape[SRC]
    nz = 8 if n == 64 else 2
    ny = n // nz
    units = n * OWN

    def on_device(design, unit_index, residual, weight, obs_count, damping):
        slots = design.shape[1]
        chunk = min(8192, slots // 2)
        dims = (nt, ny, nz, units, slots, chunk)
        vmem = pl.BlockSpec(memory_space=pltpu.VMEM)
        hbm = pl.BlockSpec(memory_space=pl.ANY)
        dma = pltpu.SemaphoreType.DMA
        sol, misfit = pl.pallas_call(
            functools.partial(kernel, dims),
            out_shape=(
                pltpu.VMEM((OWN, W), F32),
                pltpu.SMEM((1, 1), F32),
            ),
            in_specs=[hbm] * 6,
            out_specs=(vmem, pl.BlockSpec(memory_space=pltpu.SMEM)),
            scratch_shapes=[
                pltpu.VMEM((W, slots), F32),
                pltpu.VMEM((1, slots), jnp.int32),
                pltpu.VMEM((1, slots), F32),
                pltpu.VMEM((1, slots), F32),
                pltpu.SMEM((1,), jnp.int32),
                pltpu.VMEM((1, OWN), F32),
                pltpu.VMEM((units, 128), F32),
                pltpu.VMEM((units, 128), BF),
                pltpu.VMEM((units // 4, 128), BF),
                pltpu.VMEM((256, slots), BF),
                pltpu.VMEM((192, chunk), BF),
                pltpu.VMEM((units, 256), F32),
                pltpu.VMEM((units // 4, 256), F32),
                pltpu.VMEM((2, chunk), F32),
                pltpu.VMEM((n, 5, 2, 128), F32),
                pltpu.VMEM((n, 5, 2, 128), F32),
                pltpu.VMEM((152, 128), F32),
                pltpu.VMEM((1, 128), F32),
                pltpu.VMEM((n * nt, 128), F32),
                pltpu.VMEM((1, 128), F32),
                pltpu.VMEM((1, 128), F32),
                dma((slots // chunk,)),
                dma((5,)),
                dma((2,)),
                dma((2,)),
                dma, dma, dma, dma,
            ],
            compiler_params=pltpu.CompilerParams(collective_id=0, has_side_effects=True),
            name="calibrate",
        )(
            design,
            unit_index.reshape(1, slots),
            residual.reshape(1, slots),
            weight.reshape(1, slots),
            obs_count,
            damping.reshape(1, OWN),
        )
        return sol.T, misfit.reshape(())

    both = P((TM, SRC))
    return jax.shard_map(
        on_device,
        mesh=mesh,
        in_specs=(P(None, (TM, SRC)), both, both, both, both, both),
        out_specs=(P(None, (TM, SRC)), P()),
        check_vma=False,
    )
```

```python
import functools

import jax
import jax.numpy as jnp
from jax import lax
from jax.experimental import pallas as pl
from jax.experimental.pallas import tpu as pltpu
from jax.sharding import PartitionSpec as P

TM = "tm"
SRC = "src"
MESH = pl.DeviceIdType.MESH
W = 16
OWN = 8
BF = jnp.bfloat16
F32 = jnp.float32


def ring_hops(d, size):
    return min(d, size - d)


def far_first(ny, nz):
    every = [(dy, dz) for dy in range(ny) for dz in range(nz)]
    return sorted(every, key=lambda o: -(ring_hops(o[0], ny) + ring_hops(o[1], nz)))


def pair_row(i, j):
    s = j - i
    if s < 8:
        return False, s * W + i
    if s == 8:
        return True, W + i
    return False, (W - s) * W + j


def tree_sum(parts):
    while len(parts) > 1:
        parts = [sum(parts[i : i + 2][1:], parts[i]) for i in range(0, len(parts), 2)]
    return parts[0]


def kernel(
    dims,
    design_hbm, unit_hbm, resid_hbm, weight_hbm, count_hbm, damping_hbm,
    sol_ref, misfit_ref,
    design_ref, unit_ref, resid_ref, weight_ref, count_ref, damping_ref,
    line_wide, lines, rest_lines,
    feat, rest_feat, main_acc, rest_acc, sums_acc, out_box, in_box,
    table, plane_msg, plane_in, tm_msg, tm_in,
    design_sem, row_sem, box_send, box_recv, plane_send, plane_recv, tm_send, tm_recv,
):
    nt, ny, nz, units, slots, chunk = dims
    n = ny * nz
    turns = slots // chunk
    half_units = units // 2
    half_boxes = n // 2
    me_t = lax.axis_index(TM)
    me_s = lax.axis_index(SRC)
    me_y = me_s // nz
    me_z = me_s % nz

    def piece(c):
        at = pl.ds(pl.multiple_of(c * chunk, chunk), chunk)
        return pltpu.make_async_copy(design_hbm.at[:, at], design_ref.at[:, at], design_sem.at[c])

    rows = [
        pltpu.make_async_copy(a, b, row_sem.at[i])
        for i, (a, b) in enumerate(
            [
                (count_hbm, count_ref), (weight_hbm, weight_ref), (resid_hbm, resid_ref),
                (unit_hbm, unit_ref), (damping_hbm, damping_ref),
            ]
        )
    ]
    piece(0).start()
    for row in rows:
        row.start()
    for c in range(1, turns):
        piece(c).start()

    ys = [(me_y + d) % ny for d in range(ny)]
    zs = [(me_z + d) % nz for d in range(nz)]
    ts = [(me_t + d) % nt for d in range(nt)]
    order = far_first(ny, nz)

    def owner(o):
        return ys[o[0]] * nz + zs[o[1]]

    def peer(o):
        return (me_t, owner(o))

    barrier = pltpu.get_barrier_semaphore()
    for o in order[:-1]:
        pl.semaphore_signal(barrier, inc=1, device_id=peer(o), device_id_type=MESH)
    root_z = 1
    served = nz // root_z - 1
    is_root = me_z < root_z

    @pl.when(is_root)
    def _():
        def greet(place, carry):
            for d in range(1, nt):
                pl.semaphore_signal(barrier, inc=1, device_id=(ts[d], place), device_id_type=MESH)
            return carry

        lax.fori_loop(0, n, greet, 0)

    eight = lax.broadcasted_iota(jnp.int32, (OWN, 128), 0)
    for k, o in enumerate(order):
        line_wide[k * OWN : (k + 1) * OWN, :] = (eight + (owner(o) * OWN - 256)).astype(F32)
    lines[...] = line_wide[...].astype(BF)
    for k in range(0, n, 4):
        four = owner(order[k])
        for i in range(1, 4):
            four = jnp.where(eight // 2 == i, owner(order[k + i]), four)
        line_wide[2 * k : 2 * k + OWN, :] = (four * 2 + eight % 2).astype(F32)
    rest_lines[...] = line_wide[0 : 2 * n, :].astype(BF)

    main_acc[...] = jnp.zeros_like(main_acc)
    rest_acc[...] = jnp.zeros_like(rest_acc)
    sums_acc[...] = jnp.zeros_like(sums_acc)
    for row in rows:
        row.wait()
    count = count_ref[0]
    base = me_t * units

    dn = (((1,), (1,)), ((), ()))
    one, zero = jnp.ones((), BF), jnp.zeros((), BF)

    def hits(which, code):
        return jnp.where(
            jnp.concatenate([which] * (chunk // 128), axis=1) == code.astype(F32).astype(BF), one, zero
        )

    def split(value):
        hi = value.astype(BF)
        return hi, (value - hi.astype(F32)).astype(BF)

    def first_half(c, carry):
        at = pl.ds(pl.multiple_of(c * chunk, chunk), chunk)
        piece(c).wait()
        d = design_ref[:, at]
        slot = lax.broadcasted_iota(jnp.int32, (1, chunk), 1) + c * chunk
        w = jnp.where(slot < count, weight_ref[:, at], 0.0)
        r = resid_ref[:, at]
        wr = w * r
        sums_acc[0:1, :] += wr * r
        sums_acc[1:2, :] += w
        u = unit_ref[:, at] - base
        wd = d * w

        for s in range(8):
            turned = d if s == 0 else pltpu.roll(d, W - s, 0)
            hi, lo = split(wd * turned)
            feat[s * W : (s + 1) * W, at] = hi
            feat[128 + s * W : 128 + (s + 1) * W, at] = lo
        tail = jnp.concatenate([d * wr, wd[:8] * d[8:]], axis=0)
        tail_hi, tail_lo = split(tail)
        quarter = jnp.broadcast_to(
            (lax.shift_right_logical(u, 1) & 3).astype(F32), (24, chunk)
        ).astype(BF)
        for q in range(4):
            on = quarter == jnp.asarray(q, BF)
            rest_feat[q * 24 : q * 24 + 24, :] = jnp.where(on, tail_hi, zero)
            rest_feat[96 + q * 24 : 120 + q * 24, :] = jnp.where(on, tail_lo, zero)

        code = u - 256
        unit_ref[:, at] = code
        main_acc[0:half_units, :] += lax.dot_general(
            hits(lines[0:half_units, :], code), feat[:, at], dn, preferred_element_type=F32
        )
        rest_code = (lax.shift_right_logical(u, 3) * 2) | (u & 1)
        rest_acc[:, 0:192] += lax.dot_general(
            hits(rest_lines[...], rest_code), rest_feat[...], dn, preferred_element_type=F32
        )
        return carry

    def second_half(c, carry):
        at = pl.ds(pl.multiple_of(c * chunk, chunk), chunk)
        main_acc[half_units:units, :] += lax.dot_general(
            hits(lines[half_units:units, :], unit_ref[:, at]), feat[:, at], dn, preferred_element_type=F32
        )
        return carry

    def fill(h):
        got = main_acc[h * half_units : (h + 1) * half_units, :]
        out_box[h * half_boxes : (h + 1) * half_boxes, 0:4] = (
            got[:, 0:128] + got[:, 128:256]
        ).reshape(half_boxes, 4, 2, 128)

    def send(h):
        for k in range(h * half_boxes, min((h + 1) * half_boxes, n - 1)):
            pltpu.make_async_remote_copy(
                src_ref=out_box.at[k], dst_ref=in_box.at[k],
                send_sem=box_send.at[h], recv_sem=box_recv.at[h],
                device_id=peer(order[k]), device_id_type=MESH,
            ).start()

    halves = (in_box.at[0:half_boxes], in_box.at[half_boxes : n - 1])

    lax.fori_loop(0, turns, first_half, 0)
    out_box[:, 4:5] = (
        rest_acc[:, 0:128] + pltpu.roll(rest_acc[...], 160, 1)[:, 0:128]
    ).reshape(n, 1, 2, 128)
    fill(0)
    pl.semaphore_wait(barrier, n - 1 + root_z * ny * (nt - 1))
    send(0)
    lax.fori_loop(0, turns, second_half, 0)
    fill(1)
    send(1)

    before = jnp.sum(sums_acc[0:1, :], axis=1, keepdims=True)
    weight_sum = jnp.sum(sums_acc[1:2, :], axis=1, keepdims=True)
    lane_row = lax.broadcasted_iota(jnp.int32, (1, 128), 1)
    plane_msg[...] = jnp.where(
        lane_row == OWN, before, jnp.where(lane_row == OWN + 1, weight_sum, 0.0)
    )
    damping = damping_ref[...]
    own = out_box[n - 1]
    pltpu.make_async_copy(halves[0], halves[0], box_recv.at[0]).wait()
    own = tree_sum([own] + [in_box[k] for k in range(half_boxes)])
    pltpu.make_async_copy(halves[1], halves[1], box_recv.at[1]).wait()
    own = tree_sum([own] + [in_box[k] for k in range(half_boxes, n - 1)])
    main = own[0:4].reshape(OWN, 128)
    rest = own[4]
    table[0:128, :] = jnp.concatenate([main, jnp.zeros((120, 128), F32)], axis=0).T
    rest_t = jnp.concatenate([rest, jnp.zeros((126, 128), F32)], axis=0).T
    lane = lax.broadcasted_iota(jnp.int32, (24, 128), 1)
    rest_all = jnp.zeros((24, 128), F32)
    for q in range(4):
        part = rest_t[q * 24 : q * 24 + 24, :]
        moved = part if q == 0 else pltpu.roll(part, 2 * q, 1)
        rest_all = jnp.where(lane // 2 == q, moved, rest_all)
    table[128:152, :] = rest_all

    def entry(i, j):
        is_rest, row = pair_row(i, j)
        row = row + 128 if is_rest else row
        return table[row : row + 1, 0:OWN]

    a = {}
    for i in range(W):
        for j in range(i, W):
            a[i, j] = entry(i, j)
        a[i, i] = a[i, i] + damping
    b0 = [table[128 + i : 129 + i, 0:OWN] for i in range(W)]
    b = list(b0)
    inv = [None] * W
    for k in range(W):
        inv[k] = 1.0 / a[k, k]
        for j in range(k + 1, W):
            factor = a[k, j] * inv[k]
            for i in range(k + 1, j + 1):
                a[i, j] = a[i, j] - a[k, i] * factor
            b[j] = b[j] - factor * b[k]
    x = [None] * W
    for k in range(W - 1, -1, -1):
        x[k] = b[k] * inv[k]
        for i in range(k):
            b[i] = b[i] - a[i, k] * x[k]
    gain = jnp.zeros((1, OWN), F32)
    square = jnp.zeros((1, OWN), F32)
    for k in range(W):
        gain = gain + x[k] * b0[k]
        square = square + x[k] * x[k]
    plane_msg[:, 0:OWN] = -(gain + damping * square)

    def term_copy(d, dy, z):
        slot = (nt - d) % nt * n + (ny - dy) % ny * nz + (me_z - z + nz) % nz
        return pltpu.make_async_remote_copy(
            src_ref=plane_msg, dst_ref=plane_in.at[pl.ds(slot, 1)],
            send_sem=plane_send, recv_sem=plane_recv,
            device_id=(ts[d], ys[dy] * nz + z), device_id_type=MESH,
        )

    ways = sorted(
        ((d, dy) for d in range(nt) for dy in range(ny)),
        key=lambda w: -(ring_hops(w[0] // 2, nt // 2) + ring_hops(w[1], ny)),
    )
    for d, dy in ways:
        for z in range(root_z):
            if (d, dy) != (0, 0):
                term_copy(d, dy, z).start()
    for z in range(root_z):

        @pl.when(me_z != z)
        def _():
            term_copy(0, 0, z).start()

    for k in range(W):
        table[k : k + 1, 0:OWN] = x[k]
    sol_ref[...] = table[...].T[0:OWN, 0:W]
    every = n * nt - 1
    to_roots = root_z * ny * nt

    def total_copy(i):
        z = me_z + 1 + i
        return pltpu.make_async_remote_copy(
            src_ref=tm_msg, dst_ref=tm_in,
            send_sem=tm_send, recv_sem=tm_recv,
            device_id=(me_t, me_y * nz + z), device_id_type=MESH,
        )

    def finish(total):
        chi = jnp.sum(jnp.where(lane_row <= OWN, total, 0.0), axis=1, keepdims=True)
        weights = jnp.sum(jnp.where(lane_row == OWN + 1, total, 0.0), axis=1, keepdims=True)
        misfit_ref[0, 0] = jnp.sum(chi / weights)

    def drain(count, sem):
        pltpu.make_async_copy(plane_in.at[pl.ds(0, count)], plane_in.at[pl.ds(0, count)], sem).wait()

    @pl.when(is_root)
    def _():
        drain(every, plane_recv)
        plane_in[0:1] = plane_msg[...]
        eights = tree_sum([plane_in[8 * k : 8 * k + 8, :] for k in range(n * nt // 8)])
        total = jnp.sum(eights, axis=0, keepdims=True)
        tm_msg[...] = total
        for i in range(served):
            total_copy(i).start()
        finish(total)
        drain(to_roots - 1, plane_send)
        drain(served, tm_send)

    @pl.when(jnp.logical_not(is_root))
    def _():
        pltpu.make_async_copy(tm_in, tm_in, tm_recv).wait()
        finish(tm_in[...])
        drain(to_roots, plane_send)

    for h in range(2):
        pltpu.make_async_copy(halves[h], halves[h], box_send.at[h]).wait()


def solution(mesh):
    nt = mesh.shape[TM]
    n = mesh.shape[SRC]
    nz = 8 if n == 64 else 2
    ny = n // nz
    units = n * OWN

    def on_device(design, unit_index, residual, weight, obs_count, damping):
        slots = design.shape[1]
        chunk = min(8192, slots // 2)
        dims = (nt, ny, nz, units, slots, chunk)
        vmem = pl.BlockSpec(memory_space=pltpu.VMEM)
        hbm = pl.BlockSpec(memory_space=pl.ANY)
        dma = pltpu.SemaphoreType.DMA
        sol, misfit = pl.pallas_call(
            functools.partial(kernel, dims),
            out_shape=(
                pltpu.VMEM((OWN, W), F32),
                pltpu.SMEM((1, 1), F32),
            ),
            in_specs=[hbm] * 6,
            out_specs=(vmem, pl.BlockSpec(memory_space=pltpu.SMEM)),
            scratch_shapes=[
                pltpu.VMEM((W, slots), F32),
                pltpu.VMEM((1, slots), jnp.int32),
                pltpu.VMEM((1, slots), F32),
                pltpu.VMEM((1, slots), F32),
                pltpu.SMEM((1,), jnp.int32),
                pltpu.VMEM((1, OWN), F32),
                pltpu.VMEM((units, 128), F32),
                pltpu.VMEM((units, 128), BF),
                pltpu.VMEM((units // 4, 128), BF),
                pltpu.VMEM((256, slots), BF),
                pltpu.VMEM((192, chunk), BF),
                pltpu.VMEM((units, 256), F32),
                pltpu.VMEM((units // 4, 256), F32),
                pltpu.VMEM((2, chunk), F32),
                pltpu.VMEM((n, 5, 2, 128), F32),
                pltpu.VMEM((n, 5, 2, 128), F32),
                pltpu.VMEM((152, 128), F32),
                pltpu.VMEM((1, 128), F32),
                pltpu.VMEM((n * nt, 128), F32),
                pltpu.VMEM((1, 128), F32),
                pltpu.VMEM((1, 128), F32),
                dma((slots // chunk,)),
                dma((5,)),
                dma((2,)),
                dma((2,)),
                dma, dma, dma, dma,
            ],
            compiler_params=pltpu.CompilerParams(collective_id=0, has_side_effects=True),
            name="calibrate",
        )(
            design,
            unit_index.reshape(1, slots),
            residual.reshape(1, slots),
            weight.reshape(1, slots),
            obs_count,
            damping.reshape(1, OWN),
        )
        return sol.T, misfit.reshape(())

    both = P((TM, SRC))
    return jax.shard_map(
        on_device,
        mesh=mesh,
        in_specs=(P(None, (TM, SRC)), both, both, both, both, both),
        out_specs=(P(None, (TM, SRC)), P()),
        check_vma=False,
    )
```
